128 devices in a mesh: dp: 16 (over x, y), vocab: 8 (over z, core).
Axes of the slice: x: 4, y: 4, z: 4, core: 2. Of those that a mesh axis runs over, the one named last changes fastest.
Arguments:
- hidden: bfloat16 [768, 8192], P('dp', 'vocab'), may hold values from -32 to 32
- head_weight: bfloat16 [8192, 128256], P(None, ('dp', 'vocab')), may hold values from -0.9943689 to 0.9943689
- critic_in: bfloat16 [16, 8192, 4096], P('dp', None, 'vocab'), may hold values from -0.0625 to 0.0625
- critic_out: bfloat16 [16, 4096], P('dp', 'vocab'), may hold values from -0.09375 to 0.09375
- rewards: float32 [16, 12], P('dp'), may hold values from -4 to 4
- turn_ids: int32 [16, 48], P('dp'), may hold values from 0 to 11, never falling along the last dimension, each value on 1 to 8 neighbouring positions
- owners: int32 [192, 1], P('dp'), may hold values from 0 to 15; in each aligned block of 12 rows (0 to 11, 12 to 23, ...) at most 2 rows name the same one
- actions: int32 [768], replicated, may hold values from 0 to 128255
Outputs:
- hidden_grad: float32 [768, 8192], P('dp', 'vocab')
- token_logprob: float32 [768], P('dp')
- turn_advantage: float32 [16, 12], P('dp')
The draws below stay inside these ranges and needn't reach their ends.
Inputs may be any that keep to these rules, and one draw needn't show every extreme that they name: `turn_ids`: in each row, turn numbers never fall, every number of 0 to 11 appears, and each turn has 1 to 8 tokens. `owners`: among the 12 turns of one index of dp, at most 2 name the same critic, and every critic is named by some turn.
All inputs are finite; a program needn't handle non-finite values.
Results may differ from the reference program's by a relative error of at most 0.0087.
Values may be sent and summed in bfloat16 or wider, within the bound.
No kernel may reach another device: no remote copies, remote signals or barrier semaphores. Data moves between devices by JAX's collectives and lax.ppermute only.
A program may use at most 128 MiB of HBM per device.

```python
import math
import jax
import jax.numpy as jnp
import numpy as np
from jax import lax

D = 8192
V = 128256
CRIT_H = 4096
TOK_DEV = 48
TURN_DEV = 12
TURN_MOST = 8
CAP = 2
TOKENS = 768
TURNS = 192
N_DP = 16


def head_column(key, column):
    normal_part = jax.random.normal(jax.random.fold_in(jax.random.fold_in(key, 101), column), (D,), jnp.float32)
    normal_part = jnp.clip(normal_part, -6.0, 6.0) * (3.0 / math.sqrt(D))
    return normal_part


def draw_head_weight(key, part):
    columns = jax.vmap(lambda column: head_column(key, column))(jnp.arange(V, dtype=jnp.int32))
    return columns.T.astype(jnp.bfloat16)


def draw_hidden(key, part):
    normal_part = jnp.clip(jax.random.normal(jax.random.fold_in(key, 201), (TOKENS, D), jnp.float32), -6.0, 6.0)
    return jnp.clip(normal_part, -32.0, 32.0).astype(jnp.bfloat16)


def plant(entries, key, low, top_value):
    index_at = [jax.random.randint(jax.random.fold_in(key, axis), (), 0, length) for axis, length in enumerate(entries.shape)]
    longest = entries.shape.index(max(entries.shape))
    neighbour = index_at[:longest] + [(index_at[longest] + 1) % entries.shape[longest]] + index_at[longest + 1:]
    return entries.at[tuple(index_at)].set(low).at[tuple(neighbour)].set(top_value)


def levels(key, extent, pieces, low, largest):
    gain = 1.0
    for dim, blocks in pieces:
        steps = jax.random.uniform(jax.random.fold_in(jax.random.fold_in(key, 6), dim), (blocks,), jnp.float32, low / len(pieces), largest / len(pieces))
        gain = gain * jnp.repeat(jnp.exp(steps), extent[dim] // blocks).reshape((-1,) + (1,) * (len(extent) - 1 - dim))
    return gain


def ranked_wide(rng, dims, count, skew):
    portions = [min(1 << octave, count + 1 - (1 << octave)) * (1 << 20) // math.isqrt((1 << octave) ** skew) + 1 for octave in range((count + 1).bit_length()) if 1 << octave <= count]
    width = 1 + sum(portions) // (1 << 30)
    table = np.cumsum(np.array([max(1, weight // width) for weight in portions]))
    lot = jax.random.randint(jax.random.fold_in(rng, 1), dims, 0, int(table[len(portions) - 1]))
    start = jnp.left_shift(1, jnp.searchsorted(jnp.asarray(table, jnp.int32), lot, side="right").astype(jnp.int32))
    standing = start - 1 + jax.random.randint(jax.random.fold_in(rng, 4), dims, 0, 1 << 30) % jnp.minimum(start, count + 1 - start)
    return jax.random.permutation(jax.random.fold_in(rng, 2), count)[standing].astype(jnp.int32)


def profile(number_of, total, bound, lean):
    loads = [(1 << 20) // math.isqrt(rank ** lean) + 1 for rank in range(2, number_of + 1)]
    surplus, holding = total - bound - (number_of - 1), [1] * (number_of - 1)
    while surplus > 0:
        candidates = [i for i in range(number_of - 1) if holding[i] < bound]
        mass, remaining = sum([loads[i] for i in candidates]), surplus
        for i in candidates:
            more = min(bound - holding[i], max(1, remaining * loads[i] // mass), surplus)
            holding[i] = holding[i] + more
            surplus = surplus - more
    return np.array([bound] + holding)


def uneven(own_key, amount, total, limit, lean):
    if amount == 2:
        one = jax.random.randint(own_key, (), max(1, total - limit), min(limit, total - 1) + 1)
        return jnp.stack([one, total - one])
    tallies = jnp.asarray(profile(amount, total, limit, lean), jnp.int32)
    pairs = (amount - 1) // 2
    source_of, sink = tallies[1:1 + 2 * pairs:2], tallies[2:2 + 2 * pairs:2]
    room = jnp.minimum(source_of - 1, limit - sink)
    moved = jax.random.randint(jax.random.fold_in(own_key, 1), (pairs,), 0, 1 << 20) % (room + 1)
    tallies = tallies.at[1:1 + 2 * pairs:2].set(source_of - moved).at[2:2 + 2 * pairs:2].set(sink + moved)
    return tallies[jax.random.permutation(jax.random.fold_in(own_key, 2), amount)]


def routed_block(stream_key, own, number, rows, amount, top, reach, skew):
    order = jax.random.permutation(stream_key, amount)
    packed, ordinary = portions_of(amount, rows * top, reach, skew, True), portions_of(amount, rows * top, reach, skew, False)
    places = jnp.arange(amount)

    def named(sizes, offset_by):
        used = int((sizes > 0).sum())
        fixed = max(1, used // 4)
        passed = fixed + (places - fixed + offset_by * (used - fixed)) % max(1, amount - fixed)
        return jnp.zeros((amount,), jnp.int32).at[order[jnp.where(places < fixed, places, passed)]].set(jnp.asarray(sizes, jnp.int32))

    sizes = jnp.where(number % 4 == 0, named(packed, number // 4), named(ordinary, number - number // 4 - 1))
    mixed = jax.random.permutation(jax.random.fold_in(own, 3), amount)
    giver, sink = mixed[0:amount // 2 * 2:2], mixed[1:amount // 2 * 2:2]
    room = jnp.minimum(sizes[giver] - 1, reach - sizes[sink]) // 2
    room = jnp.where((giver == order[0]) | (sink == order[0]) | (sizes[sink] == 0), 0, jnp.maximum(room, 0))
    passed = jax.random.randint(jax.random.fold_in(own, 4), (amount // 2,), 0, 1 << 20) % (room + 1)
    sizes = sizes.at[giver].add(-passed).at[sink].add(passed)
    labels = jnp.searchsorted(jnp.cumsum(sizes), jnp.arange(rows * top), side="right").astype(jnp.int32)
    listing = labels.reshape(top, rows).T
    listing = listing[jax.random.permutation(jax.random.fold_in(own, 1), rows)]
    offset_by = jax.random.randint(jax.random.fold_in(own, 2), (rows, 1), 0, top)
    return jnp.take_along_axis(listing, (jnp.arange(top)[None, :] + offset_by) % top, axis=1)


def portions_of(count, total, bound, slope, full):
    loads = [(1 << 20) // math.isqrt(rank ** slope) + 1 for rank in range(1, count + 1)]
    largest = bound if full else min(bound, max(-(-total // count), total * loads[0] // sum(loads)))
    least = 1 if total - largest >= count - 1 else 0
    holding, surplus = [largest] + [least] * (count - 1), total - largest - least * (count - 1)
    while surplus > 0:
        movable = [i for i in range(1, count) if holding[i] < largest] or [i for i in range(1, count) if holding[i] < bound]
        mass, remaining = sum([loads[i] for i in movable]), surplus
        for i in movable:
            addition = min(bound - holding[i], max(1, remaining * loads[i] // mass), surplus)
            holding[i] = holding[i] + addition
            surplus = surplus - addition
    return np.array(holding)


def noise(key, dims, deviation, bound, pieces=(), kind=jnp.bfloat16):
    entries = deviation * jax.random.normal(key, dims, jnp.float32)
    if pieces:
        entries = entries * levels(key, dims, pieces, -0.22, 0.18)
    return jnp.clip(entries, -bound, bound).astype(kind)


def setup_inputs(seed: int = 0) -> dict:
    streams_of = jax.random.split(jax.random.key(seed), 9)
    hidden = draw_hidden(jax.random.fold_in(streams_of[8], 71), 0)
    head_weight = draw_head_weight(jax.random.fold_in(streams_of[8], 71), 0)
    critic_in = noise(streams_of[2], (N_DP, D, CRIT_H), D ** -0.5, 0.0625, ((0, 16), (2, 8)))
    critic_out = noise(streams_of[3], (N_DP, CRIT_H), CRIT_H ** -0.5, 0.09375, ((0, 16), (1, 8)))
    rewards = noise(streams_of[4], (N_DP, TURN_DEV), 1.0, 4.0, ((0, 16),), jnp.float32)
    turn_ids = jax.vmap(lambda own: jnp.searchsorted(jnp.cumsum(uneven(own, TURN_DEV, TOK_DEV, TURN_MOST, 1)), jnp.arange(TOK_DEV), side="right"))(jax.random.split(streams_of[5], N_DP)).reshape((N_DP, TOK_DEV)).astype(jnp.int32)
    owners_keys = jax.random.split(jax.random.fold_in(streams_of[6], 1), TURNS // TURN_DEV)
    owners_turns = jax.random.permutation(jax.random.fold_in(streams_of[6], 3), TURNS // TURN_DEV)
    owners = jax.vmap(lambda own, number: routed_block(jax.random.fold_in(streams_of[6], 2), own, number, TURN_DEV, N_DP, 1, CAP, 2))(owners_keys, owners_turns).reshape((TURNS, 1))
    actions = plant(ranked_wide(streams_of[7], (TOKENS,), V, 1), jax.random.fold_in(streams_of[7], 3), 0, V - 1).astype(jnp.int32)
    return {"hidden": hidden, "head_weight": head_weight, "critic_in": critic_in, "critic_out": critic_out, "rewards": rewards, "turn_ids": turn_ids, "owners": owners, "actions": actions}


epsilon = 1e-05
loss_scale = 32.0

def rms_norm(values):
    return values * lax.rsqrt(lax.optimization_barrier(jnp.mean(values * values, axis=-1, keepdims=True)) + epsilon)

def reference(hidden, head_weight, critic_in, critic_out, rewards, turn_ids, owners, actions):
    position = jnp.arange(TOK_DEV, dtype=jnp.int32)
    turn_range = jnp.arange(TURN_DEV, dtype=jnp.int32)
    member = turn_ids[:, None, :] == turn_range[None, :, None]
    last_pos = lax.optimization_barrier(jnp.max(jnp.where(member, position[None, None, :], -1), axis=2))
    end_pick = (position[None, None, :] == last_pos[:, :, None]).astype(jnp.float32)
    shard_hidden = hidden.astype(jnp.float32).reshape(N_DP, TOK_DEV, D)
    end_rows = jnp.einsum('pti,pid->ptd', end_pick, shard_hidden, precision=lax.Precision.HIGHEST)
    end_rows = end_rows.reshape(TURNS, D)
    owner_of = owners[:, 0].astype(jnp.int32)

    def score(item):
        row_values, index = item
        normed = rms_norm(row_values[None, :]).astype(jnp.bfloat16)
        inner = jnp.dot(normed, critic_in[index], preferred_element_type=jnp.float32)
        active = jax.nn.silu(inner).astype(jnp.bfloat16)
        return jnp.dot(active, critic_out[index][:, None], preferred_element_type=jnp.float32)[0, 0]
    turn_value = lax.map(score, (end_rows, owner_of))
    advantage = rewards - turn_value.reshape(N_DP, TURN_DEV)
    token_adv = lax.optimization_barrier(jnp.sum(jnp.where(member, advantage[:, :, None], 0.0), axis=1)).reshape(TOKENS)
    logits = jnp.dot(hidden, head_weight, preferred_element_type=jnp.float32)
    row_top = lax.optimization_barrier(jnp.max(logits, axis=1))
    shifted = jnp.exp(logits - row_top[:, None])
    row_mass = lax.optimization_barrier(jnp.sum(shifted, axis=1))
    vocab_range = jnp.arange(V, dtype=jnp.int32)
    hit = vocab_range[None, :] == actions[:, None]
    picked = lax.optimization_barrier(jnp.sum(jnp.where(hit, logits, 0.0), axis=1))
    logprob = picked - row_top - jnp.log(row_mass)
    grad_logits = (loss_scale * token_adv[:, None] * (shifted / row_mass[:, None] - hit.astype(jnp.float32))).astype(jnp.bfloat16)
    hidden_grad = lax.dot_general(grad_logits, head_weight, (((1,), (1,)), ((), ())), preferred_element_type=jnp.float32)
    return (hidden_grad, logprob, advantage)
```

```python
import jax
import jax.numpy as jnp
from jax import lax
from jax.sharding import Mesh
from jax.sharding import PartitionSpec as P

DP = ("dp_0", "dp_1")
VOCAB = ("vocab_0", "vocab_1")
DP_VOCAB = ("dp_0", "dp_1", "vocab_0", "vocab_1")


epsilon = 1e-05
loss_scale = 32.0


def sent_to_all(x, axis):
    size = lax.axis_size(axis)
    return lax.all_to_all(jnp.broadcast_to(x[None], (size, *x.shape)), axis, 0, 0, tiled=True)


def in_order(parts, dim):
    parts = jnp.moveaxis(parts, 0, dim)
    shape = parts.shape
    return parts.reshape(*shape[:dim], shape[dim] * shape[dim + 1], *shape[dim + 2 :])


def gather_directly(x, axis, dim):
    parts = sent_to_all(x, axis)
    return in_order(parts, dim)


def over_copies(x, axis):
    return sent_to_all(x, axis).sum(axis=0)


def merged_over(stats, axis):
    both = sent_to_all(jnp.stack(stats), axis)
    tops = both[:, 0]
    top = jnp.max(tops, axis=0)
    mass = jnp.sum(both[:, 1] * jnp.exp(tops - top[None, :]), axis=0)
    return (top, mass, jnp.sum(both[:, 2], axis=0))


def in_blocks(x, dim, size):
    before, after = (x.shape[:dim], x.shape[dim + 1 :])
    return jnp.moveaxis(x.reshape(*before, size, -1, *after), dim, 0)


def summed_on_arrival(x, axis, dim):
    size = lax.axis_size(axis)
    parts = lax.all_to_all(in_blocks(x, dim, size), axis, 0, 0, tiled=True)
    return jnp.sum(parts.astype(jnp.float32), axis=0)


def rms_norm(values):
    return values * lax.rsqrt(jnp.mean(values * values, axis=-1, keepdims=True) + epsilon)


def on_device(hidden, head_weight, critic_in, critic_out, rewards, turn_ids, owners, actions):
    ranks_dp = lax.axis_size(DP)
    ranks_vocab = lax.axis_size(VOCAB)
    tok_dev = hidden.shape[0]
    turn_dev = rewards.shape[1]
    slot_count = max(2, 2 * turn_dev // ranks_dp)
    vocab_local = head_weight.shape[1]
    position = jnp.arange(tok_dev, dtype=jnp.int32)
    turn_range = jnp.arange(turn_dev, dtype=jnp.int32)
    member = turn_ids[0][None, :] == turn_range[:, None]
    last_pos = jnp.max(jnp.where(member, position[None, :], -1), axis=1)
    end_pick = (position[None, :] == last_pos[:, None]).astype(jnp.bfloat16)
    owner_of = owners[:, 0]
    earlier = (owner_of[None, :] == owner_of[:, None]) & (turn_range[None, :] < turn_range[:, None])
    slot_of = jnp.sum(earlier.astype(jnp.int32), axis=1)
    dest_range = jnp.arange(ranks_dp, dtype=jnp.int32)
    slot_range = jnp.arange(slot_count, dtype=jnp.int32)
    dispatch = (owner_of[:, None, None] == dest_range[None, :, None]) & (
        slot_of[:, None, None] == slot_range[None, None, :]
    )
    route_matrix = dispatch.reshape(turn_dev, ranks_dp * slot_count).astype(jnp.bfloat16)
    end_slices = jnp.dot(end_pick, hidden, preferred_element_type=jnp.float32).astype(jnp.bfloat16)
    outgoing = jnp.dot(route_matrix.T, end_slices, preferred_element_type=jnp.float32).astype(
        jnp.bfloat16
    )
    outgoing = outgoing.reshape(ranks_dp, slot_count, hidden.shape[1])
    whole_rows = gather_directly(
        lax.all_to_all(outgoing, DP, split_axis=0, concat_axis=0, tiled=True), VOCAB, 2
    )
    flat_rows = whole_rows.reshape(-1, whole_rows.shape[2]).astype(jnp.float32)
    normed = rms_norm(flat_rows).astype(jnp.bfloat16)
    inner = jnp.dot(normed, critic_in[0], preferred_element_type=jnp.float32)
    active = jax.nn.silu(inner).astype(jnp.bfloat16)
    partial_value = jnp.dot(active, critic_out[0], preferred_element_type=jnp.float32)
    summed_value = over_copies(partial_value, VOCAB)
    values = lax.all_to_all(
        summed_value.reshape(whole_rows.shape[0], whole_rows.shape[1]),
        DP,
        split_axis=0,
        concat_axis=0,
        tiled=True,
    )
    turn_value = jnp.sum(jnp.where(dispatch, values[None, :, :], 0.0), axis=(1, 2))
    advantage = rewards[0] - turn_value
    token_adv = jnp.sum(jnp.where(member, advantage[:, None], 0.0), axis=0)
    spread = lax.all_gather(hidden, DP_VOCAB, axis=0, tiled=False)
    spread = spread.reshape(ranks_dp, ranks_vocab, tok_dev, hidden.shape[1])
    split_weight = head_weight.reshape(ranks_vocab, hidden.shape[1], vocab_local)
    logits = lax.dot_general(
        spread,
        split_weight,
        (((1, 3), (0, 1)), ((), ())),
        preferred_element_type=jnp.float32,
    ).reshape(ranks_dp * tok_dev, vocab_local)
    first_col = (lax.axis_index(DP) * ranks_vocab + lax.axis_index(VOCAB)) * vocab_local
    local_action = actions - first_col
    hit = jnp.arange(vocab_local, dtype=jnp.int32)[None, :] == local_action[:, None]
    picked_part = jnp.sum(jnp.where(hit, logits, 0.0), axis=1)
    local_top = jnp.max(logits, axis=1)
    local_mass = jnp.sum(jnp.exp(logits - local_top[:, None]), axis=1)
    row_top, row_mass, picked = merged_over(
        merged_over((local_top, local_mass, picked_part), VOCAB), DP
    )
    logprob_all = picked - row_top - jnp.log(row_mass)
    token_logprob = lax.dynamic_slice_in_dim(logprob_all, lax.axis_index(DP) * tok_dev, tok_dev, 0)
    probs = jnp.exp(logits - row_top[:, None]) / row_mass[:, None]
    grad_logits = (probs - hit.astype(jnp.float32)).astype(jnp.bfloat16)
    summed = lax.psum_scatter(
        lax.dot_general(
            head_weight, grad_logits, (((1,), (1,)), ((), ())), preferred_element_type=jnp.float32
        ).astype(jnp.bfloat16),
        VOCAB,
        scatter_dimension=0,
        tiled=True,
    )
    hidden_grad = summed_on_arrival(summed, DP, 1).T * (loss_scale * token_adv[:, None])
    return (hidden_grad, token_logprob, advantage[None, :])


def solution(mesh):
    finer = Mesh(mesh.devices.reshape(4, 4, 4, 2), ("dp_0", "dp_1", "vocab_0", "vocab_1"))
    return jax.shard_map(
        on_device,
        mesh=finer,
        in_specs=(
            P(DP, VOCAB),
            P(None, DP_VOCAB),
            P(DP, None, VOCAB),
            P(DP, VOCAB),
            P(DP, None),
            P(DP, None),
            P(DP, None),
            P(),
        ),
        out_specs=(P(DP, VOCAB), P(DP), P(DP, None)),
        check_vma=False,
    )
```

```python
import functools

import jax
import jax.numpy as jnp
from jax import lax
from jax.experimental import pallas as pl
from jax.experimental.pallas import tpu as pltpu
from jax.sharding import Mesh
from jax.sharding import PartitionSpec as P


DP = ("dp_0", "dp_1")
VOCAB = ("vocab_0", "vocab_1")
DP_VOCAB = ("dp_0", "dp_1", "vocab_0", "vocab_1")
X, Y, Z, CORE = DP_VOCAB
SIDE = 4
LANES = 128
CHUNK = 256


epsilon = 1e-05
loss_scale = 32.0
f32 = jnp.float32
bf16 = jnp.bfloat16


def from_ahead(x, axis, k):
    return lax.ppermute(x, axis, [((i + k) % SIDE, i) for i in range(SIDE)])


def to_ahead(x, axis, k):
    return lax.ppermute(x, axis, [(i, (i + k) % SIDE) for i in range(SIDE)])


def to_partner(x):
    return lax.ppermute(x, CORE, [(0, 1), (1, 0)])


def over(x, axis):
    return lax.all_to_all(x, axis, 0, 0, tiled=True)


def to_lines(flat, lines):
    return jnp.pad(flat, (0, lines * LANES - flat.shape[0])).reshape(lines, LANES)


def gathered(hidden):
    ahead = [hidden] + [from_ahead(hidden, Z, k) for k in (1, 3, 2)]
    low = jnp.stack([ahead[0], ahead[1]])
    high = jnp.stack([ahead[3], ahead[2]])
    low_x = [low] + [from_ahead(low, X, k) for k in (1, 3, 2)]
    high_y = [high] + [from_ahead(high, Y, k) for k in (1, 3, 2)]
    low = jnp.stack([low_x[0], low_x[1], low_x[3], low_x[2]])
    high = jnp.stack([high_y[0], high_y[1], high_y[3], high_y[2]])
    a = {0: low} | {k: from_ahead(low, Y, k) for k in (1, 3, 2)}
    b = {0: high} | {k: from_ahead(high, X, k) for k in (1, 3, 2)}
    return [a[k] for k in range(SIDE)], [b[k] for k in range(SIDE)]


def logits_body(place, *refs):
    pieces = refs[:16]
    weight, critic, score, pick, local = refs[16:21]
    logits, stats, value = refs[21:24]
    rows, inner, squares = refs[24:]
    step = pl.program_id(0)
    tok = pieces[0].shape[2]
    for own in range(2):
        for grp in range(2):

            @pl.when(step // 2 == own * 2 + grp)
            def _(own=own, grp=grp):
                for k in range(SIDE):
                    piece = pieces[own * 8 + grp * 4 + k]
                    for j in range(SIDE):
                        at = (k * SIDE + j if grp == 0 else j * SIDE + k) * tok
                        rows[at : at + tok] = piece[j, 0]

    @pl.when(step == 0)
    def _():
        logits[...] = jnp.zeros(logits.shape, f32)
        inner[...] = jnp.zeros(inner.shape, f32)
        squares[...] = jnp.zeros(squares.shape, f32)

    for at in range(0, rows.shape[0], CHUNK):
        logits[:, at : at + CHUNK] += lax.dot_general(
            weight[...], rows[at : at + CHUNK], (((1,), (1,)), ((), ())), preferred_element_type=f32
        )
    ends = lax.dot_general(
        pick[...], rows[...], (((1,), (0,)), ((), ())), preferred_element_type=f32
    )
    inner[...] += jnp.dot(ends.astype(bf16), critic[0], preferred_element_type=f32)
    squares[...] += jnp.sum(ends * ends, axis=1, keepdims=True)

    @pl.when(step == 7)
    def _():
        full = logits[...]
        top = jnp.max(full, axis=0, keepdims=True)
        stats[0:1] = top
        stats[1:2] = jnp.sum(jnp.exp(full - top), axis=0, keepdims=True)
        ids = lax.broadcasted_iota(jnp.int32, full.shape, 0)
        stats[2:3] = jnp.sum(jnp.where(ids == local[0:1], full, 0.0), axis=0, keepdims=True)
        stats[3:8] = jnp.zeros((5, full.shape[1]), f32)
        mean = squares[:, :1] / (weight.shape[1] * 8)
        hid = inner[...] * lax.rsqrt(mean + epsilon)
        active = (hid / (1.0 + jnp.exp(-hid))).astype(bf16).astype(f32)
        out = jnp.sum(active * score[...].astype(f32), axis=1, keepdims=True)
        value[...] = jnp.broadcast_to(out, value.shape)


def feature_block(place, dz, other):
    return ((place[0] + dz) % SIDE) * 2 + (place[1] + other) % 2


def find_logits(place, pieces, weight, critic_in, critic_out, pick, local):
    vocab, _ = weight.shape
    tok, feat = pieces[0].shape[2:]
    hidden_units = critic_in.shape[2]
    slots, tokens = pick.shape

    def piece_spec(own, grp):
        first = own * 4 + grp * 2
        return pl.BlockSpec(
            (SIDE, 1, tok, feat), lambda s, p: (0, jnp.where(s > first, 1, 0), 0, 0)
        )

    whole = lambda shape: pl.BlockSpec(shape, lambda s, p: (0,) * len(shape))
    specs = [piece_spec(own, grp) for own in range(2) for grp in range(2) for _ in range(SIDE)]
    specs += [
        pl.BlockSpec((vocab, feat), lambda s, p: (0, feature_block(p, s % 4, s // 4))),
        pl.BlockSpec((1, feat, hidden_units), lambda s, p: (0, feature_block(p, s % 4, s // 4), 0)),
        whole((1, hidden_units)),
        whole((slots, tokens)),
        whole((8, tokens)),
    ]
    return pl.pallas_call(
        logits_body,
        grid_spec=pltpu.PrefetchScalarGridSpec(
            num_scalar_prefetch=1,
            grid=(8,),
            in_specs=specs,
            out_specs=[whole((vocab, tokens)), whole((8, tokens)), whole((slots, LANES))],
            scratch_shapes=[
                pltpu.VMEM((tokens, feat), bf16),
                pltpu.VMEM((slots, hidden_units), f32),
                pltpu.VMEM((slots, LANES), f32),
            ],
        ),
        out_shape=[
            jax.ShapeDtypeStruct((vocab, tokens), f32),
            jax.ShapeDtypeStruct((8, tokens), f32),
            jax.ShapeDtypeStruct((slots, LANES), f32),
        ],
        compiler_params=pltpu.CompilerParams(
            dimension_semantics=("arbitrary",), vmem_limit_bytes=56 * 2**20
        ),
        name="logits",
    )(place, *pieces, weight, critic_in, critic_out, pick, local)


def first_body(place, logits, stats, local, weight, grad, out, turned):
    vocab = logits.shape[0]

    @pl.when(pl.program_id(0) == 0)
    def _():
        ids = lax.broadcasted_iota(jnp.int32, logits.shape, 0)
        hit = jnp.where(ids == local[0:1], 1.0, 0.0)
        probs = jnp.exp(logits[...] - stats[0:1]) / stats[1:2]
        turned[vocab // 16 * 16 :] = jnp.zeros(
            (turned.shape[0] - vocab // 16 * 16, turned.shape[1]), bf16
        )
        turned[:vocab] = (probs - hit).astype(bf16)
        grad[...] = jnp.transpose(turned[...])[:, :vocab]

    out[0] = jnp.dot(grad[...], weight[...], preferred_element_type=f32).astype(bf16)


def next_body(place, grad, weight, out):
    out[0] = jnp.dot(grad[...], weight[...], preferred_element_type=f32).astype(bf16)


def last_body(grp, place, grad, weight, other, *outs):
    tok = outs[0].shape[2]
    both = jnp.dot(grad[...], weight[...], preferred_element_type=f32) + other[0].astype(f32)
    both = both.astype(bf16)
    for k in range(SIDE):
        for j in range(SIDE):
            at = (k * SIDE + j if grp == 0 else j * SIDE + k) * tok
            outs[k][j, 0] = both[at : at + tok]


def back(place, weight, grp, other_core, tok, feat, grad=None, softmax=None, received=None):
    vocab = weight.shape[0]
    tokens = SIDE * SIDE * tok
    whole = lambda shape: pl.BlockSpec(shape, lambda s, p: (0,) * len(shape))
    weight_spec = pl.BlockSpec(
        (vocab, feat), lambda s, p: (0, feature_block(p, s + 2 * grp, other_core))
    )
    tile = pl.BlockSpec((1, tokens, feat), lambda s, p: (s, 0, 0))
    tile_shape = jax.ShapeDtypeStruct((2, tokens, feat), bf16)
    scratch = []
    if softmax is not None:
        body = first_body
        args = (*softmax, weight)
        in_specs = [whole((vocab, tokens)), whole((8, tokens)), whole((8, tokens)), weight_spec]
        scratch = [pltpu.VMEM((-(-vocab // LANES) * LANES, tokens), bf16)]
        out_specs = [whole((tokens, vocab)), tile]
        out_shape = [jax.ShapeDtypeStruct((tokens, vocab), bf16), tile_shape]
    elif received is None:
        body = next_body
        args = (grad, weight)
        in_specs = [whole((tokens, vocab)), weight_spec]
        out_specs = [tile]
        out_shape = [tile_shape]
    else:
        body = functools.partial(last_body, grp)
        args = (grad, weight, received)
        in_specs = [whole((tokens, vocab)), weight_spec, tile]
        piece = pl.BlockSpec((SIDE, 1, tok, feat), lambda s, p: (0, s, 0, 0))
        out_specs = [piece] * SIDE
        out_shape = [jax.ShapeDtypeStruct((SIDE, 2, tok, feat), bf16)] * SIDE
    return pl.pallas_call(
        body,
        grid_spec=pltpu.PrefetchScalarGridSpec(
            num_scalar_prefetch=1,
            grid=(2,),
            in_specs=in_specs,
            out_specs=out_specs,
            scratch_shapes=scratch,
        ),
        out_shape=out_shape,
        compiler_params=pltpu.CompilerParams(
            dimension_semantics=("arbitrary",), vmem_limit_bytes=56 * 2**20
        ),
    )(place, *args)


def added(parts):
    total = parts[0].astype(f32)
    for part in parts[1:]:
        total = total + part.astype(f32)
    return total


def sent_and_added(pieces, axis):
    return added([pieces[0]] + [to_ahead(pieces[k], axis, k) for k in (1, 3, 2)])


def on_device(hidden, head_weight, critic_in, critic_out, rewards, turn_ids, owners, actions):
    tok_dev, feat = hidden.shape
    turn_dev = rewards.shape[1]
    ranks_dp = SIDE * SIDE
    tokens = ranks_dp * tok_dev
    slot_count = max(2, 2 * turn_dev // ranks_dp)
    slots = ranks_dp * slot_count
    vocab_local = head_weight.shape[1]
    weight = head_weight.T
    at_x, at_y, at_z, at_core = (lax.axis_index(axis) for axis in DP_VOCAB)
    place = jnp.stack([at_z, at_core]).astype(jnp.int32)

    def ahead_order(v):
        v = v.reshape(*v.shape[:-1], SIDE, SIDE, tok_dev)
        v = jnp.roll(jnp.roll(v, -at_x, axis=-3), -at_y, axis=-2)
        return jnp.swapaxes(v, -3, -2).reshape(*v.shape[:-3], tokens)

    def true_order(v):
        v = jnp.swapaxes(v.reshape(*v.shape[:-1], SIDE, SIDE, tok_dev), -3, -2)
        v = jnp.roll(jnp.roll(v, at_x, axis=-3), at_y, axis=-2)
        return v.reshape(*v.shape[:-3], tokens)

    low, high = gathered(hidden)
    pieces = low + high
    pieces = pieces + [to_partner(p) for p in pieces]

    position = jnp.arange(tok_dev, dtype=jnp.int32)
    turn_range = jnp.arange(turn_dev, dtype=jnp.int32)
    member = turn_ids[0][None, :] == turn_range[:, None]
    last_pos = jnp.max(jnp.where(member, position[None, :], -1), axis=1)
    owner_of = owners[:, 0]
    earlier = (owner_of[None, :] == owner_of[:, None]) & (turn_range[None, :] < turn_range[:, None])
    slot_of = jnp.sum(earlier.astype(jnp.int32), axis=1)
    dest_range = jnp.arange(ranks_dp, dtype=jnp.int32)
    slot_range = jnp.arange(slot_count, dtype=jnp.int32)
    dispatch = (owner_of[:, None, None] == dest_range[None, :, None]) & (
        slot_of[:, None, None] == slot_range[None, None, :]
    )
    spots = jnp.max(jnp.where(dispatch, last_pos[:, None, None], -1), axis=0).astype(f32)
    spots, _ = lax.optimization_barrier((spots, low[0]))
    wanted = over(spots, DP).reshape(slots).astype(jnp.int32)
    order = jnp.arange(tokens, dtype=jnp.int32)
    block_y = (order // (SIDE * tok_dev) + at_y) % SIDE
    block_x = (order // tok_dev % SIDE + at_x) % SIDE
    block = block_x * SIDE + block_y
    slot_range_all = jnp.arange(slots, dtype=jnp.int32)
    pick = (
        (slot_range_all[:, None] // slot_count == block[None, :])
        & (wanted[:, None] == (order % tok_dev)[None, :])
    ).astype(bf16)

    first_col = (lax.axis_index(DP) * (2 * SIDE) + at_z * 2 + at_core) * vocab_local
    local = jnp.broadcast_to(ahead_order(actions - first_col)[None], (8, tokens))

    logits, stats, value = find_logits(
        place, pieces, weight, critic_in, critic_out, pick, local
    )

    lines = (3 * tokens + slots + LANES - 1) // LANES
    message = to_lines(jnp.concatenate([stats[:3].reshape(-1), value[:, 0]]), lines)
    both = over(jnp.broadcast_to(message[None], (2 * SIDE, *message.shape)), VOCAB)
    both = both.reshape(2 * SIDE, -1)
    tops = both[:, :tokens]
    masses = both[:, tokens : 2 * tokens]
    top = jnp.max(tops, axis=0)
    mass = jnp.sum(masses * jnp.exp(tops - top[None]), axis=0)
    picked = jnp.sum(both[:, 2 * tokens : 3 * tokens], axis=0)
    values = jnp.sum(both[:, 3 * tokens : 3 * tokens + slots], axis=0)
    straight = true_order(jnp.stack([top, mass, picked]))
    shared = jnp.broadcast_to(straight[:2].reshape(1, -1), (ranks_dp, 2 * tokens))
    message = jnp.concatenate(
        [shared, straight[2].reshape(ranks_dp, tok_dev), values.reshape(ranks_dp, slot_count)],
        axis=1,
    )
    width = -(-message.shape[1] // LANES) * LANES
    message = jnp.pad(message, ((0, 0), (0, width - message.shape[1])))
    both = over(message.reshape(ranks_dp, -1, LANES), DP).reshape(ranks_dp, width)
    tops = both[:, :tokens]
    masses = both[:, tokens : 2 * tokens]
    top = jnp.max(tops, axis=0)
    mass = jnp.sum(masses * jnp.exp(tops - top[None]), axis=0)
    picked = jnp.sum(both[:, 2 * tokens : 2 * tokens + tok_dev], axis=0)
    values = both[:, 2 * tokens + tok_dev : 2 * tokens + tok_dev + slot_count]
    ordered = ahead_order(jnp.stack([top, mass]))
    token_logprob = picked - ordered[0, :tok_dev] - jnp.log(ordered[1, :tok_dev])
    turn_value = jnp.sum(jnp.where(dispatch, values[None], 0.0), axis=(1, 2))
    advantage = rewards[0] - turn_value
    token_adv = jnp.sum(jnp.where(member, advantage[:, None], 0.0), axis=0)

    softmax = (logits, jnp.pad(ordered, ((0, 6), (0, 0))), local)
    grad, out_low = back(place, weight, 0, 1, tok_dev, feat, softmax=softmax)
    in_low = to_partner(out_low)
    (out_high,) = back(place, weight, 1, 1, tok_dev, feat, grad=grad)
    in_high = to_partner(out_high)
    low = back(place, weight, 0, 0, tok_dev, feat, grad=grad, received=in_low)
    high = back(place, weight, 1, 0, tok_dev, feat, grad=grad, received=in_high)
    low = sent_and_added(low, Y).astype(bf16)
    high = sent_and_added(high, X).astype(bf16)
    low = sent_and_added([low[k] for k in range(SIDE)], X).astype(bf16)
    high = sent_and_added([high[k] for k in range(SIDE)], Y).astype(bf16)
    total = sent_and_added([low[0], low[1], high[0], high[1]], Z)
    hidden_grad = total * (loss_scale * token_adv[:, None])
    return (hidden_grad, token_logprob, advantage[None, :])


def solution(mesh):
    finer = Mesh(mesh.devices.reshape(4, 4, 4, 2), DP_VOCAB)

    return jax.shard_map(
        on_device,
        mesh=finer,
        in_specs=(
            P(DP, VOCAB),
            P(None, DP_VOCAB),
            P(DP, None, VOCAB),
            P(DP, VOCAB),
            P(DP, None),
            P(DP, None),
            P(DP, None),
            P(),
        ),
        out_specs=(P(DP, VOCAB), P(DP), P(DP, None)),
        check_vma=False,
    )
```

```python
import functools

import jax
import jax.numpy as jnp
from jax import lax
from jax.experimental import pallas as pl
from jax.experimental.pallas import tpu as pltpu
from jax.sharding import Mesh
from jax.sharding import PartitionSpec as P

DP = ("dp_0", "dp_1")
VOCAB = ("vocab_0", "vocab_1")
DP_VOCAB = ("dp_0", "dp_1", "vocab_0", "vocab_1")
X, Y, Z, CORE = DP_VOCAB
SIDE = 4
LANES = 128
CHUNK = 256


epsilon = 1e-05
loss_scale = 32.0
f32 = jnp.float32
bf16 = jnp.bfloat16


def from_ahead(x, axis, k):
    return lax.ppermute(x, axis, [((i + k) % SIDE, i) for i in range(SIDE)])


def to_ahead(x, axis, k):
    return lax.ppermute(x, axis, [(i, (i + k) % SIDE) for i in range(SIDE)])


def to_partner(x):
    return lax.ppermute(x, CORE, [(0, 1), (1, 0)])


def over(x, axis):
    return lax.all_to_all(x, axis, 0, 0, tiled=True)


def to_lines(flat, lines):
    return jnp.pad(flat, (0, lines * LANES - flat.shape[0])).reshape(lines, LANES)


def gathered(hidden, table):
    ahead = [hidden] + [from_ahead(hidden, Z, k) for k in (1, 3, 2)]
    table = jnp.stack([table] + [from_ahead(table, X, k) for k in (1, 2, 3)])
    low = jnp.stack([ahead[0], ahead[1]])
    high = jnp.stack([ahead[3], ahead[2]])
    low, high, table = lax.optimization_barrier((low, high, table))
    low_x = [low] + [from_ahead(low, X, k) for k in (1, 3, 2)]
    table = jnp.stack([table] + [from_ahead(table, Y, k) for k in (1, 2, 3)])
    high_y = [high] + [from_ahead(high, Y, k) for k in (1, 3, 2)]
    low = jnp.stack([low_x[0], low_x[1], low_x[3], low_x[2]])
    high = jnp.stack([high_y[0], high_y[1], high_y[3], high_y[2]])
    low, high, table = lax.optimization_barrier((low, high, table))
    a = {0: low} | {k: from_ahead(low, Y, k) for k in (1, 3, 2)}
    b = {0: high} | {k: from_ahead(high, X, k) for k in (1, 3, 2)}
    return [a[k] for k in range(SIDE)], [b[k] for k in range(SIDE)], table


def logits_body(final, place, *refs):
    pieces = refs[:8]
    weight, critic, pick = refs[8:11]
    if final:
        logits_in, inner_in, squares_in, score, local = refs[11:16]
        logits, stats, value, rows, inner, squares = refs[16:]
    else:
        logits, inner, squares, rows = refs[11:]
    step = pl.program_id(0)
    tok = pieces[0].shape[2]
    for grp in range(2):

        @pl.when(step // 2 == grp)
        def _(grp=grp):
            for k in range(SIDE):
                for j in range(SIDE):
                    at = (k * SIDE + j if grp == 0 else j * SIDE + k) * tok
                    rows[at : at + tok] = pieces[grp * 4 + k][j, 0]

    @pl.when(step == 0)
    def _():
        if final:
            logits[...] = logits_in[...]
            inner[...] = inner_in[...]
            squares[...] = squares_in[...]
        else:
            logits[...] = jnp.zeros(logits.shape, f32)
            inner[...] = jnp.zeros(inner.shape, f32)
            squares[...] = jnp.zeros(squares.shape, f32)

    for at in range(0, rows.shape[0], CHUNK):
        logits[:, at : at + CHUNK] += lax.dot_general(
            weight[...], rows[at : at + CHUNK], (((1,), (1,)), ((), ())), preferred_element_type=f32
        )
    ends = lax.dot_general(
        pick[...], rows[...], (((1,), (0,)), ((), ())), preferred_element_type=f32
    )
    inner[...] += jnp.dot(ends.astype(bf16), critic[0], preferred_element_type=f32)
    squares[...] += jnp.sum(ends * ends, axis=1, keepdims=True)
    if not final:
        return

    @pl.when(step == 3)
    def _():
        full = logits[...]
        top = jnp.max(full, axis=0, keepdims=True)
        stats[0:1] = top
        stats[1:2] = jnp.sum(jnp.exp(full - top), axis=0, keepdims=True)
        ids = lax.broadcasted_iota(jnp.int32, full.shape, 0)
        stats[2:3] = jnp.sum(jnp.where(ids == local[0:1], full, 0.0), axis=0, keepdims=True)
        stats[3:8] = jnp.zeros((5, full.shape[1]), f32)
        mean = squares[:, :1] / (weight.shape[1] * 8)
        hid = inner[...] * lax.rsqrt(mean + epsilon)
        active = (hid / (1.0 + jnp.exp(-hid))).astype(bf16).astype(f32)
        out = jnp.sum(active * score[...].astype(f32), axis=1, keepdims=True)
        value[...] = jnp.broadcast_to(out, value.shape)


def feature_block(place, dz, other):
    return ((place[0] + dz) % SIDE) * 2 + (place[1] + other) % 2


def find_logits(place, other, pieces, weight, critic_in, pick, before=None, rest=None):
    vocab, wide = weight.shape
    tok, feat = pieces[0].shape[2:]
    hidden_units = critic_in.shape[2]
    slots, tokens = pick.shape
    piece_spec = lambda grp: pl.BlockSpec(
        (SIDE, 1, tok, feat), lambda s, p: (0, jnp.where(s > 2 * grp, 1, 0), 0, 0)
    )
    whole = lambda shape: pl.BlockSpec(shape, lambda s, p: (0,) * len(shape))
    specs = [piece_spec(grp) for grp in range(2) for _ in range(SIDE)]
    specs += [
        pl.BlockSpec((vocab, feat), lambda s, p: (0, feature_block(p, s, other))),
        pl.BlockSpec((1, feat, hidden_units), lambda s, p: (0, feature_block(p, s, other), 0)),
        whole((slots, tokens)),
    ]
    sums = [(vocab, tokens), (slots, hidden_units), (slots, LANES)]
    scratch = [pltpu.VMEM((tokens, feat), bf16)]
    args = (*pieces, weight, critic_in, pick)
    if before is None:
        outs = sums
    else:
        args += (*before, *rest)
        specs += [whole(v.shape) for v in (*before, *rest)]
        outs = [(vocab, tokens), (8, tokens), (slots, LANES)]
        scratch += [pltpu.VMEM(shape, f32) for shape in sums[1:]]
    return pl.pallas_call(
        functools.partial(logits_body, before is not None),
        grid_spec=pltpu.PrefetchScalarGridSpec(
            num_scalar_prefetch=1,
            grid=(4,),
            in_specs=specs,
            out_specs=[whole(shape) for shape in outs],
            scratch_shapes=scratch,
        ),
        out_shape=[jax.ShapeDtypeStruct(shape, f32) for shape in outs],
        compiler_params=pltpu.CompilerParams(
            dimension_semantics=("arbitrary",), vmem_limit_bytes=56 * 2**20
        ),
        name=f"logits_{other}",
    )(place, *args)


def first_body(place, logits, stats, local, weight, grad, out, turned):
    vocab = logits.shape[0]

    @pl.when(pl.program_id(0) == 0)
    def _():
        ids = lax.broadcasted_iota(jnp.int32, logits.shape, 0)
        hit = jnp.where(ids == local[0:1], 1.0, 0.0)
        probs = jnp.exp(logits[...] - stats[0:1]) / stats[1:2]
        turned[vocab // 16 * 16 :] = jnp.zeros(
            (turned.shape[0] - vocab // 16 * 16, turned.shape[1]), bf16
        )
        turned[:vocab] = (probs - hit).astype(bf16)
        grad[...] = jnp.transpose(turned[...])[:, :vocab]

    out[0] = jnp.dot(grad[...], weight[...], preferred_element_type=f32).astype(bf16)


def next_body(place, grad, weight, out):
    out[0] = jnp.dot(grad[...], weight[...], preferred_element_type=f32).astype(bf16)


def last_body(grp, place, grad, weight, other, *outs):
    tok = outs[0].shape[2]
    both = jnp.dot(grad[...], weight[...], preferred_element_type=f32) + other[0].astype(f32)
    both = both.astype(bf16)
    for k in range(SIDE):
        for j in range(SIDE):
            at = (k * SIDE + j if grp == 0 else j * SIDE + k) * tok
            outs[k][j, 0] = both[at : at + tok]


def back(place, weight, grp, other_core, tok, feat, grad=None, softmax=None, received=None):
    vocab = weight.shape[0]
    tokens = SIDE * SIDE * tok
    whole = lambda shape: pl.BlockSpec(shape, lambda s, p: (0,) * len(shape))
    weight_spec = pl.BlockSpec(
        (vocab, feat), lambda s, p: (0, feature_block(p, s + 2 * grp, other_core))
    )
    tile = pl.BlockSpec((1, tokens, feat), lambda s, p: (s, 0, 0))
    tile_shape = jax.ShapeDtypeStruct((2, tokens, feat), bf16)
    scratch = []
    if softmax is not None:
        body = first_body
        args = (*softmax, weight)
        in_specs = [whole((vocab, tokens)), whole((8, tokens)), whole((8, tokens)), weight_spec]
        scratch = [pltpu.VMEM((-(-vocab // LANES) * LANES, tokens), bf16)]
        out_specs = [whole((tokens, vocab)), tile]
        out_shape = [jax.ShapeDtypeStruct((tokens, vocab), bf16), tile_shape]
    elif received is None:
        body = next_body
        args = (grad, weight)
        in_specs = [whole((tokens, vocab)), weight_spec]
        out_specs = [tile]
        out_shape = [tile_shape]
    else:
        body = functools.partial(last_body, grp)
        args = (grad, weight, received)
        in_specs = [whole((tokens, vocab)), weight_spec, tile]
        piece = pl.BlockSpec((SIDE, 1, tok, feat), lambda s, p: (0, s, 0, 0))
        out_specs = [piece] * SIDE
        out_shape = [jax.ShapeDtypeStruct((SIDE, 2, tok, feat), bf16)] * SIDE
    return pl.pallas_call(
        body,
        grid_spec=pltpu.PrefetchScalarGridSpec(
            num_scalar_prefetch=1,
            grid=(2,),
            in_specs=in_specs,
            out_specs=out_specs,
            scratch_shapes=scratch,
        ),
        out_shape=out_shape,
        compiler_params=pltpu.CompilerParams(
            dimension_semantics=("arbitrary",), vmem_limit_bytes=56 * 2**20
        ),
        name=f"back_{grp}_{other_core}",
    )(place, *args)


def added(parts):
    total = parts[0].astype(f32)
    for part in parts[1:]:
        total = total + part.astype(f32)
    return total


def sent_and_added(pieces, axis):
    return added([pieces[0]] + [to_ahead(pieces[k], axis, k) for k in (1, 3, 2)])


def on_device(hidden, head_weight, critic_in, critic_out, rewards, turn_ids, owners, actions):
    tok_dev, feat = hidden.shape
    turn_dev = rewards.shape[1]
    ranks_dp = SIDE * SIDE
    tokens = ranks_dp * tok_dev
    slot_count = max(2, 2 * turn_dev // ranks_dp)
    slots = ranks_dp * slot_count
    vocab_local = head_weight.shape[1]
    weight = head_weight.T
    at_x, at_y, at_z, at_core = (lax.axis_index(axis) for axis in DP_VOCAB)
    place = jnp.stack([at_z, at_core]).astype(jnp.int32)

    def ahead_order(v):
        v = v.reshape(*v.shape[:-1], SIDE, SIDE, tok_dev)
        v = jnp.roll(jnp.roll(v, -at_x, axis=-3), -at_y, axis=-2)
        return jnp.swapaxes(v, -3, -2).reshape(*v.shape[:-3], tokens)

    def true_order(v):
        v = jnp.swapaxes(v.reshape(*v.shape[:-1], SIDE, SIDE, tok_dev), -3, -2)
        v = jnp.roll(jnp.roll(v, at_x, axis=-3), at_y, axis=-2)
        return v.reshape(*v.shape[:-3], tokens)

    position = jnp.arange(tok_dev, dtype=jnp.int32)
    turn_range = jnp.arange(turn_dev, dtype=jnp.int32)
    member = turn_ids[0][None, :] == turn_range[:, None]
    last_pos = jnp.max(jnp.where(member, position[None, :], -1), axis=1)
    owner_of = owners[:, 0]
    earlier = (owner_of[None, :] == owner_of[:, None]) & (turn_range[None, :] < turn_range[:, None])
    slot_of = jnp.sum(earlier.astype(jnp.int32), axis=1)
    dest_range = jnp.arange(ranks_dp, dtype=jnp.int32)
    slot_range = jnp.arange(slot_count, dtype=jnp.int32)
    dispatch = (owner_of[:, None, None] == dest_range[None, :, None]) & (
        slot_of[:, None, None] == slot_range[None, None, :]
    )
    spots = jnp.max(jnp.where(dispatch, last_pos[:, None, None], -1), axis=0).astype(f32)
    wanted = to_lines(spots.reshape(-1), 8)
    low, high, wanted = gathered(hidden, wanted)
    pieces = low + high
    partner = [to_partner(p) for p in pieces]
    wanted = wanted[:, :, 0, :slots].reshape(ranks_dp, ranks_dp, slot_count)
    mine = (dest_range == at_x * SIDE + at_y)[None, :, None]
    wanted = jnp.max(jnp.where(mine, wanted, -1.0), axis=1).astype(jnp.int32).reshape(slots)
    order = jnp.arange(tokens, dtype=jnp.int32)
    slot_range_all = jnp.arange(slots, dtype=jnp.int32)
    pick = (
        (slot_range_all[:, None] // slot_count == (order // tok_dev)[None, :])
        & (wanted[:, None] == (order % tok_dev)[None, :])
    ).astype(bf16)

    first_col = (lax.axis_index(DP) * (2 * SIDE) + at_z * 2 + at_core) * vocab_local
    local = jnp.broadcast_to(ahead_order(actions - first_col)[None], (8, tokens))

    before = find_logits(place, 0, pieces, weight, critic_in, pick)
    logits, stats, value = find_logits(
        place, 1, partner, weight, critic_in, pick, before, (critic_out, local)
    )

    lines = (3 * tokens + slots + LANES - 1) // LANES
    message = to_lines(jnp.concatenate([stats[:3].reshape(-1), value[:, 0]]), lines)
    both = over(jnp.broadcast_to(message[None], (2 * SIDE, *message.shape)), VOCAB)
    both = both.reshape(2 * SIDE, -1)
    tops = both[:, :tokens]
    masses = both[:, tokens : 2 * tokens]
    top = jnp.max(tops, axis=0)
    mass = jnp.sum(masses * jnp.exp(tops - top[None]), axis=0)
    picked = jnp.sum(both[:, 2 * tokens : 3 * tokens], axis=0)
    values = jnp.sum(both[:, 3 * tokens : 3 * tokens + slots], axis=0)
    values = jnp.swapaxes(values.reshape(SIDE, SIDE, slot_count), 0, 1)
    values = jnp.roll(jnp.roll(values, at_x, axis=0), at_y, axis=1).reshape(ranks_dp, slot_count)
    straight = true_order(jnp.stack([top, mass, picked]))
    shared = jnp.broadcast_to(straight[:2].reshape(1, -1), (ranks_dp, 2 * tokens))
    message = jnp.concatenate(
        [shared, straight[2].reshape(ranks_dp, tok_dev), values],
        axis=1,
    )
    width = -(-message.shape[1] // LANES) * LANES
    message = jnp.pad(message, ((0, 0), (0, width - message.shape[1])))
    both = over(message.reshape(ranks_dp, -1, LANES), DP).reshape(ranks_dp, width)
    tops = both[:, :tokens]
    masses = both[:, tokens : 2 * tokens]
    top = jnp.max(tops, axis=0)
    mass = jnp.sum(masses * jnp.exp(tops - top[None]), axis=0)
    picked = jnp.sum(both[:, 2 * tokens : 2 * tokens + tok_dev], axis=0)
    values = both[:, 2 * tokens + tok_dev : 2 * tokens + tok_dev + slot_count]
    ordered = ahead_order(jnp.stack([top, mass]))
    token_logprob = picked - ordered[0, :tok_dev] - jnp.log(ordered[1, :tok_dev])
    turn_value = jnp.sum(jnp.where(dispatch, values[None], 0.0), axis=(1, 2))
    advantage = rewards[0] - turn_value
    token_adv = jnp.sum(jnp.where(member, advantage[:, None], 0.0), axis=0)

    softmax = (logits, jnp.pad(ordered, ((0, 6), (0, 0))), local)
    grad, out_low = back(place, weight, 0, 1, tok_dev, feat, softmax=softmax)
    in_low = to_partner(out_low)
    (out_high,) = back(place, weight, 1, 1, tok_dev, feat, grad=grad)
    in_high = to_partner(out_high)
    low = back(place, weight, 0, 0, tok_dev, feat, grad=grad, received=in_low)
    high = back(place, weight, 1, 0, tok_dev, feat, grad=grad, received=in_high)
    low = sent_and_added(low, Y).astype(bf16)
    high = sent_and_added(high, X).astype(bf16)
    low = sent_and_added([low[k] for k in range(SIDE)], X).astype(bf16)
    high = sent_and_added([high[k] for k in range(SIDE)], Y).astype(bf16)
    total = sent_and_added([low[0], low[1], high[0], high[1]], Z)
    hidden_grad = total * (loss_scale * token_adv[:, None])
    return (hidden_grad, token_logprob, advantage[None, :])


def solution(mesh):
    finer = Mesh(mesh.devices.reshape(4, 4, 4, 2), DP_VOCAB)

    return jax.shard_map(
        on_device,
        mesh=finer,
        in_specs=(
            P(DP, VOCAB),
            P(None, DP_VOCAB),
            P(DP, None, VOCAB),
            P(DP, VOCAB),
            P(DP, None),
            P(DP, None),
            P(DP, None),
            P(),
        ),
        out_specs=(P(DP, VOCAB), P(DP), P(DP, None)),
        check_vma=False,
    )
```

```python
import functools

import jax
import jax.numpy as jnp
from jax import lax
from jax.experimental import pallas as pl
from jax.experimental.pallas import tpu as pltpu
from jax.sharding import Mesh
from jax.sharding import PartitionSpec as P

DP = ("dp_0", "dp_1")
VOCAB = ("vocab_0", "vocab_1")
DP_VOCAB = ("dp_0", "dp_1", "vocab_0", "vocab_1")
X, Y, Z, CORE = DP_VOCAB
SIDE = 4
LANES = 128
CHUNK = 256


GATHER = ((0, 0, 4), (1, 0, 4), (3, 0, 4), (2, 0, 2), (2, 2, 2))
SCATTER = ((0, 0, 4), (2, 0, 2), (2, 2, 2), (1, 2, 2), (3, 0, 2), (1, 0, 2), (3, 2, 2))

epsilon = 1e-05
loss_scale = 32.0
f32 = jnp.float32
bf16 = jnp.bfloat16


def from_ahead(x, axis, k):
    return lax.ppermute(x, axis, [((i + k) % SIDE, i) for i in range(SIDE)])


def to_ahead(x, axis, k):
    return lax.ppermute(x, axis, [(i, (i + k) % SIDE) for i in range(SIDE)])


def to_partner(x):
    return lax.ppermute(x, CORE, [(0, 1), (1, 0)])


def over(x, axis):
    return lax.all_to_all(x, axis, 0, 0, tiled=True)


def to_lines(flat, lines):
    return jnp.pad(flat, (0, lines * LANES - flat.shape[0])).reshape(lines, LANES)


def gathered(hidden, table):
    ahead = [hidden] + [from_ahead(hidden, Z, k) for k in (1, 3, 2)]
    table = jnp.stack([table] + [from_ahead(table, X, k) for k in (1, 2, 3)])
    low = jnp.stack([ahead[0], ahead[1]])
    high = jnp.stack([ahead[3], ahead[2]])
    low, high, table = lax.optimization_barrier((low, high, table))
    low_x = [low] + [from_ahead(low, X, k) for k in (1, 3, 2)]
    table = jnp.stack([table] + [from_ahead(table, Y, k) for k in (1, 2, 3)])
    high_y = [high] + [from_ahead(high, Y, k) for k in (1, 3, 2)]
    low = jnp.stack([low_x[0], low_x[1], low_x[3], low_x[2]])
    high = jnp.stack([high_y[0], high_y[1], high_y[3], high_y[2]])
    low, high, table = lax.optimization_barrier((low, high, table))
    near = [(from_ahead(v, axis, 1), from_ahead(v, axis, 3)) for v, axis in ((low, Y), (high, X))]
    out = []
    for v, axis, (up, down) in ((low, Y, near[0]), (high, X, near[1])):
        half = SIDE // 2
        out += [v, up, down, from_ahead(up[:half], axis, 1), from_ahead(down[half:], axis, 3)]
    return out, table


def logits_body(final, place, *refs):
    count = 2 * len(GATHER)
    pieces = refs[:count]
    weight, critic, pick = refs[count : count + 3]
    refs = refs[count + 3 :]
    if final:
        logits_in, inner_in, squares_in, score, local = refs[:5]
        logits, stats, value, rows, inner, squares = refs[5:]
    else:
        logits, inner, squares, rows = refs
    step = pl.program_id(0)
    tok = pieces[0].shape[2]
    for grp in range(2):

        @pl.when(step // 2 == grp)
        def _(grp=grp):
            for n, (k, first, blocks) in enumerate(GATHER):
                for j in range(first, first + blocks):
                    at = (k * SIDE + j if grp == 0 else j * SIDE + k) * tok
                    rows[at : at + tok] = pieces[grp * len(GATHER) + n][j - first, 0]

    @pl.when(step == 0)
    def _():
        if final:
            logits[...] = logits_in[...]
            inner[...] = inner_in[...]
            squares[...] = squares_in[...]
        else:
            logits[...] = jnp.zeros(logits.shape, f32)
            inner[...] = jnp.zeros(inner.shape, f32)
            squares[...] = jnp.zeros(squares.shape, f32)

    @pl.loop(0, rows.shape[0] // CHUNK)
    def _(n):
        at = pl.ds(pl.multiple_of(n * CHUNK, CHUNK), CHUNK)
        logits[:, at] += lax.dot_general(
            weight[...], rows[at], (((1,), (1,)), ((), ())), preferred_element_type=f32
        )

    ends = lax.dot_general(
        pick[...], rows[...], (((1,), (0,)), ((), ())), preferred_element_type=f32
    )
    inner[...] += jnp.dot(ends.astype(bf16), critic[0], preferred_element_type=f32)
    squares[...] += jnp.sum(ends * ends, axis=1, keepdims=True)
    if not final:
        return

    @pl.when(step == 3)
    def _():
        full = logits[...]
        top = jnp.max(full, axis=0, keepdims=True)
        stats[0:1] = top
        stats[1:2] = jnp.sum(jnp.exp(full - top), axis=0, keepdims=True)
        ids = lax.broadcasted_iota(jnp.int32, full.shape, 0)
        stats[2:3] = jnp.sum(jnp.where(ids == local[0:1], full, 0.0), axis=0, keepdims=True)
        stats[3:8] = jnp.zeros((5, full.shape[1]), f32)
        mean = squares[:, :1] / (weight.shape[1] * 8)
        hid = inner[...] * lax.rsqrt(mean + epsilon)
        active = (hid / (1.0 + jnp.exp(-hid))).astype(bf16).astype(f32)
        out = jnp.sum(active * score[...].astype(f32), axis=1, keepdims=True)
        value[...] = jnp.broadcast_to(out, value.shape)


def feature_block(place, dz, other):
    return ((place[0] + dz) % SIDE) * 2 + (place[1] + other) % 2


def find_logits(place, other, pieces, weight, critic_in, pick, before=None, rest=None):
    vocab, wide = weight.shape
    tok, feat = pieces[0].shape[2:]
    hidden_units = critic_in.shape[2]
    slots, tokens = pick.shape
    piece_spec = lambda grp, blocks: pl.BlockSpec(
        (blocks, 1, tok, feat), lambda s, p: (0, jnp.where(s > 2 * grp, 1, 0), 0, 0)
    )
    whole = lambda shape: pl.BlockSpec(shape, lambda s, p: (0,) * len(shape))
    specs = [piece_spec(grp, blocks) for grp in range(2) for _, _, blocks in GATHER]
    specs += [
        pl.BlockSpec((vocab, feat), lambda s, p: (0, feature_block(p, s, other))),
        pl.BlockSpec((1, feat, hidden_units), lambda s, p: (0, feature_block(p, s, other), 0)),
        whole((slots, tokens)),
    ]
    sums = [(vocab, tokens), (slots, hidden_units), (slots, LANES)]
    scratch = [pltpu.VMEM((tokens, feat), bf16)]
    args = (*pieces, weight, critic_in, pick)
    if before is None:
        outs = sums
    else:
        args += (*before, *rest)
        specs += [whole(v.shape) for v in (*before, *rest)]
        outs = [(vocab, tokens), (8, tokens), (slots, LANES)]
        scratch += [pltpu.VMEM(shape, f32) for shape in sums[1:]]
    return pl.pallas_call(
        functools.partial(logits_body, before is not None),
        grid_spec=pltpu.PrefetchScalarGridSpec(
            num_scalar_prefetch=1,
            grid=(4,),
            in_specs=specs,
            out_specs=[whole(shape) for shape in outs],
            scratch_shapes=scratch,
        ),
        out_shape=[jax.ShapeDtypeStruct(shape, f32) for shape in outs],
        compiler_params=pltpu.CompilerParams(
            dimension_semantics=("arbitrary",), vmem_limit_bytes=56 * 2**20
        ),
        name=f"logits_{other}",
    )(place, *args)


def first_body(place, logits, stats, local, weight, grad, out, turned):
    vocab = logits.shape[0]

    @pl.when(pl.program_id(0) == 0)
    def _():
        ids = lax.broadcasted_iota(jnp.int32, logits.shape, 0)
        hit = jnp.where(ids == local[0:1], 1.0, 0.0)
        probs = jnp.exp(logits[...] - stats[0:1]) / stats[1:2]
        turned[vocab // 16 * 16 :] = jnp.zeros(
            (turned.shape[0] - vocab // 16 * 16, turned.shape[1]), bf16
        )
        turned[:vocab] = (probs - hit).astype(bf16)
        grad[...] = jnp.transpose(turned[...])[:, :vocab]

    out[0] = jnp.dot(grad[...], weight[...], preferred_element_type=f32).astype(bf16)


def next_body(place, grad, weight, out):
    out[0] = jnp.dot(grad[...], weight[...], preferred_element_type=f32).astype(bf16)


def last_body(grp, place, grad, weight, other, *outs):
    tok = outs[0].shape[2]
    both = jnp.dot(grad[...], weight[...], preferred_element_type=f32) + other[0].astype(f32)
    both = both.astype(bf16)
    for n, (k, first, blocks) in enumerate(SCATTER):
        for j in range(first, first + blocks):
            at = (k * SIDE + j if grp == 0 else j * SIDE + k) * tok
            outs[n][j - first, 0] = both[at : at + tok]


def back(place, weight, grp, other_core, tok, feat, grad=None, softmax=None, received=None):
    vocab = weight.shape[0]
    tokens = SIDE * SIDE * tok
    whole = lambda shape: pl.BlockSpec(shape, lambda s, p: (0,) * len(shape))
    weight_spec = pl.BlockSpec(
        (vocab, feat), lambda s, p: (0, feature_block(p, s + 2 * grp, other_core))
    )
    tile = pl.BlockSpec((1, tokens, feat), lambda s, p: (s, 0, 0))
    tile_shape = jax.ShapeDtypeStruct((2, tokens, feat), bf16)
    scratch = []
    if softmax is not None:
        body = first_body
        args = (*softmax, weight)
        in_specs = [whole((vocab, tokens)), whole((8, tokens)), whole((8, tokens)), weight_spec]
        scratch = [pltpu.VMEM((-(-vocab // LANES) * LANES, tokens), bf16)]
        out_specs = [whole((tokens, vocab)), tile]
        out_shape = [jax.ShapeDtypeStruct((tokens, vocab), bf16), tile_shape]
    elif received is None:
        body = next_body
        args = (grad, weight)
        in_specs = [whole((tokens, vocab)), weight_spec]
        out_specs = [tile]
        out_shape = [tile_shape]
    else:
        body = functools.partial(last_body, grp)
        args = (grad, weight, received)
        in_specs = [whole((tokens, vocab)), weight_spec, tile]
        out_specs = [
            pl.BlockSpec((blocks, 1, tok, feat), lambda s, p: (0, s, 0, 0))
            for _, _, blocks in SCATTER
        ]
        out_shape = [
            jax.ShapeDtypeStruct((blocks, 2, tok, feat), bf16) for _, _, blocks in SCATTER
        ]
    return pl.pallas_call(
        body,
        grid_spec=pltpu.PrefetchScalarGridSpec(
            num_scalar_prefetch=1,
            grid=(2,),
            in_specs=in_specs,
            out_specs=out_specs,
            scratch_shapes=scratch,
        ),
        out_shape=out_shape,
        compiler_params=pltpu.CompilerParams(
            dimension_semantics=("arbitrary",), vmem_limit_bytes=56 * 2**20
        ),
        name=f"back_{grp}_{other_core}",
    )(place, *args)


def added(parts):
    total = parts[0].astype(f32)
    for part in parts[1:]:
        total = total + part.astype(f32)
    return total


def sent_and_added(pieces, axis):
    return added([pieces[0]] + [to_ahead(pieces[k], axis, k) for k in (1, 3, 2)])


def relayed(pieces, axis):
    kept, two_front, two_back, up_back, down_front, up_front, down_back = pieces
    half = kept.shape[0] // 2
    passing_up = to_ahead(two_front, axis, 1)
    passing_down = to_ahead(two_back, axis, 3)
    up_back = to_ahead(up_back, axis, 1)
    down_front = to_ahead(down_front, axis, 3)
    up_front = to_ahead(added([up_front, passing_up]).astype(bf16), axis, 1)
    down_back = to_ahead(added([down_back, passing_down]).astype(bf16), axis, 3)
    front = added([kept[:half], up_front, down_front]).astype(bf16)
    back_half = added([kept[half:], up_back, down_back]).astype(bf16)
    return [v[k] for v in (front, back_half) for k in range(half)]


def on_device(hidden, head_weight, critic_in, critic_out, rewards, turn_ids, owners, actions):
    tok_dev, feat = hidden.shape
    turn_dev = rewards.shape[1]
    ranks_dp = SIDE * SIDE
    tokens = ranks_dp * tok_dev
    slot_count = max(2, 2 * turn_dev // ranks_dp)
    slots = ranks_dp * slot_count
    vocab_local = head_weight.shape[1]
    weight = head_weight.T
    at_x, at_y, at_z, at_core = (lax.axis_index(axis) for axis in DP_VOCAB)
    place = jnp.stack([at_z, at_core]).astype(jnp.int32)

    def ahead_order(v):
        v = v.reshape(*v.shape[:-1], SIDE, SIDE, tok_dev)
        v = jnp.roll(jnp.roll(v, -at_x, axis=-3), -at_y, axis=-2)
        return jnp.swapaxes(v, -3, -2).reshape(*v.shape[:-3], tokens)

    def true_order(v):
        v = jnp.swapaxes(v.reshape(*v.shape[:-1], SIDE, SIDE, tok_dev), -3, -2)
        v = jnp.roll(jnp.roll(v, at_x, axis=-3), at_y, axis=-2)
        return v.reshape(*v.shape[:-3], tokens)

    position = jnp.arange(tok_dev, dtype=jnp.int32)
    turn_range = jnp.arange(turn_dev, dtype=jnp.int32)
    member = turn_ids[0][None, :] == turn_range[:, None]
    last_pos = jnp.max(jnp.where(member, position[None, :], -1), axis=1)
    owner_of = owners[:, 0]
    earlier = (owner_of[None, :] == owner_of[:, None]) & (turn_range[None, :] < turn_range[:, None])
    slot_of = jnp.sum(earlier.astype(jnp.int32), axis=1)
    dest_range = jnp.arange(ranks_dp, dtype=jnp.int32)
    slot_range = jnp.arange(slot_count, dtype=jnp.int32)
    dispatch = (owner_of[:, None, None] == dest_range[None, :, None]) & (
        slot_of[:, None, None] == slot_range[None, None, :]
    )
    spots = jnp.max(jnp.where(dispatch, last_pos[:, None, None], -1), axis=0).astype(f32)
    wanted = to_lines(spots.reshape(-1), 8)
    pieces, wanted = gathered(hidden, wanted)
    partner = [to_partner(p) for p in pieces]
    wanted = wanted[:, :, 0, :slots].reshape(ranks_dp, ranks_dp, slot_count)
    mine = (dest_range == at_x * SIDE + at_y)[None, :, None]
    wanted = jnp.max(jnp.where(mine, wanted, -1.0), axis=1).astype(jnp.int32).reshape(slots)
    order = jnp.arange(tokens, dtype=jnp.int32)
    slot_range_all = jnp.arange(slots, dtype=jnp.int32)
    pick = (
        (slot_range_all[:, None] // slot_count == (order // tok_dev)[None, :])
        & (wanted[:, None] == (order % tok_dev)[None, :])
    ).astype(bf16)

    first_col = (lax.axis_index(DP) * (2 * SIDE) + at_z * 2 + at_core) * vocab_local
    local = jnp.broadcast_to(ahead_order(actions - first_col)[None], (8, tokens))

    before = find_logits(place, 0, pieces, weight, critic_in, pick)
    logits, stats, value = find_logits(
        place, 1, partner, weight, critic_in, pick, before, (critic_out, local)
    )

    lines = (3 * tokens + slots + LANES - 1) // LANES
    message = to_lines(jnp.concatenate([stats[:3].reshape(-1), value[:, 0]]), lines)
    both = over(jnp.broadcast_to(message[None], (2 * SIDE, *message.shape)), VOCAB)
    both = both.reshape(2 * SIDE, -1)
    tops = both[:, :tokens]
    masses = both[:, tokens : 2 * tokens]
    top = jnp.max(tops, axis=0)
    mass = jnp.sum(masses * jnp.exp(tops - top[None]), axis=0)
    picked = jnp.sum(both[:, 2 * tokens : 3 * tokens], axis=0)
    values = jnp.sum(both[:, 3 * tokens : 3 * tokens + slots], axis=0)
    values = jnp.swapaxes(values.reshape(SIDE, SIDE, slot_count), 0, 1)
    values = jnp.roll(jnp.roll(values, at_x, axis=0), at_y, axis=1).reshape(ranks_dp, slot_count)
    straight = true_order(jnp.stack([top, mass, picked]))
    shared = jnp.broadcast_to(straight[:2].reshape(1, -1), (ranks_dp, 2 * tokens))
    message = jnp.concatenate(
        [shared, straight[2].reshape(ranks_dp, tok_dev), values],
        axis=1,
    )
    width = -(-message.shape[1] // LANES) * LANES
    message = jnp.pad(message, ((0, 0), (0, width - message.shape[1])))
    both = over(message.reshape(ranks_dp, -1, LANES), DP).reshape(ranks_dp, width)
    tops = both[:, :tokens]
    masses = both[:, tokens : 2 * tokens]
    top = jnp.max(tops, axis=0)
    mass = jnp.sum(masses * jnp.exp(tops - top[None]), axis=0)
    picked = jnp.sum(both[:, 2 * tokens : 2 * tokens + tok_dev], axis=0)
    values = both[:, 2 * tokens + tok_dev : 2 * tokens + tok_dev + slot_count]
    ordered = ahead_order(jnp.stack([top, mass]))
    token_logprob = picked - ordered[0, :tok_dev] - jnp.log(ordered[1, :tok_dev])
    turn_value = jnp.sum(jnp.where(dispatch, values[None], 0.0), axis=(1, 2))
    advantage = rewards[0] - turn_value
    token_adv = jnp.sum(jnp.where(member, advantage[:, None], 0.0), axis=0)

    softmax = (logits, jnp.pad(ordered, ((0, 6), (0, 0))), local)
    grad, out_low = back(place, weight, 0, 1, tok_dev, feat, softmax=softmax)
    in_low = to_partner(out_low)
    (out_high,) = back(place, weight, 1, 1, tok_dev, feat, grad=grad)
    in_high = to_partner(out_high)
    low = back(place, weight, 0, 0, tok_dev, feat, grad=grad, received=in_low)
    high = back(place, weight, 1, 0, tok_dev, feat, grad=grad, received=in_high)
    low = relayed(low, Y)
    high = relayed(high, X)
    low = sent_and_added(low, X).astype(bf16)
    high = sent_and_added(high, Y).astype(bf16)
    total = sent_and_added([low[0], low[1], high[0], high[1]], Z)
    hidden_grad = total * (loss_scale * token_adv[:, None])
    return (hidden_grad, token_logprob, advantage[None, :])


def solution(mesh):
    finer = Mesh(mesh.devices.reshape(4, 4, 4, 2), DP_VOCAB)

    return jax.shard_map(
        on_device,
        mesh=finer,
        in_specs=(
            P(DP, VOCAB),
            P(None, DP_VOCAB),
            P(DP, None, VOCAB),
            P(DP, VOCAB),
            P(DP, None),
            P(DP, None),
            P(DP, None),
            P(),
        ),
        out_specs=(P(DP, VOCAB), P(DP), P(DP, None)),
        check_vma=False,
    )
```
